32 devices in a mesh: seq: 8 (over z, y), dp: 4 (over x, core).
Axes of the slice: x: 2, y: 2, z: 4, core: 2. Of those that a mesh axis runs over, the one named last changes fastest.
Arguments:
- queries: bfloat16 [4, 2048, 2048], P('dp', 'seq'), may hold values from -12 to 12
- keys: bfloat16 [4, 2048, 1024], P('dp', 'seq'), may hold values from -6 to 6
- values: bfloat16 [4, 2048, 1024], P('dp', 'seq'), may hold values from -6 to 6
- out_grad: bfloat16 [4, 2048, 1792], P('dp', 'seq'), may hold values from -6 to 6
- out_weight: bfloat16 [2048, 1792], P('seq'), may hold values from -0.125 to 0.125
- seq_len: int32 [4], P('dp'), may hold values from 512 to 2048, as said below
Outputs:
- query_grad: bfloat16 [4, 2048, 2048], P('dp', 'seq')
- key_grad: bfloat16 [4, 2048, 1024], P('dp', 'seq')
- value_grad: bfloat16 [4, 2048, 1024], P('dp', 'seq')
- weight_grad: float32 [2048, 1792], P('seq')
- grad_rms: float32 [], replicated
The draws below stay inside these ranges and needn't reach their ends.
Inputs may be any that keep to these rules, and one draw needn't show every extreme that they name: `seq_len`: at least one sequence has the full length 2048.
All inputs are finite; a program needn't handle non-finite values.
Results may differ from the reference program's by a relative error of at most 0.014.
Values may be sent and summed in bfloat16 or wider, within the bound.
A program may use at most 128 MiB of HBM per device.

```python
import jax
import jax.numpy as jnp
from jax import lax

HEADS = 8
KV_HEADS = 4
HEAD_DIM = 256
D_OUT = 1792
WINDOW = 512
TOK_DEV = 256
SEQ = 2048
N_SEQ = 8
N_DP = 4


def draw_seq_len(key, part):
    total = TOK_DEV * N_SEQ
    lengths = jax.random.randint(jax.random.fold_in(key, 11), (N_DP,), total // 4, total + 1, dtype=jnp.int32)
    chosen = jax.random.randint(jax.random.fold_in(key, 12), (), 0, N_DP, dtype=jnp.int32)
    places = jnp.arange(N_DP, dtype=jnp.int32)
    return jnp.where(places == chosen, jnp.int32(total), lengths).astype(jnp.int32)


def level_of(rng, extent, cuts, least, top_value):
    loudness, own = 1.0, jax.random.fold_in(rng, 6)
    for axis_at, shards_of in cuts:
        draws = jnp.exp(jax.random.uniform(jax.random.fold_in(own, axis_at), (shards_of,), jnp.float32, least / len(cuts), top_value / len(cuts)))
        loudness = loudness * jnp.repeat(draws, extent[axis_at] // shards_of).reshape([-1 if axis == axis_at else 1 for axis in range(len(extent))])
    return loudness


def scatter_about(stream_key, dims, width, most, split=(), kind=jnp.bfloat16):
    values = jax.random.normal(stream_key, dims, jnp.float32) * width
    if len(split) > 0:
        values = level_of(stream_key, dims, split, -0.22, 0.18) * values
    return jnp.clip(values, min=-most, max=most).astype(kind)


def setup_inputs(seed: int = 0) -> dict:
    arg_keys = jax.random.split(jax.random.key(seed), 7)
    queries = scatter_about(arg_keys[0], (N_DP, SEQ, HEADS * HEAD_DIM), 2.0, 12.0, ((0, 4), (1, 8)))
    keys = scatter_about(arg_keys[1], (N_DP, SEQ, KV_HEADS * HEAD_DIM), 1.0, 6.0, ((0, 4), (1, 8)))
    values = scatter_about(arg_keys[2], (N_DP, SEQ, KV_HEADS * HEAD_DIM), 1.0, 6.0, ((0, 4), (1, 8)))
    out_grad = scatter_about(arg_keys[3], (N_DP, SEQ, D_OUT), 1.0, 6.0, ((0, 4), (1, 8)))
    out_weight = scatter_about(arg_keys[4], (HEADS * HEAD_DIM, D_OUT), (HEADS * HEAD_DIM) ** -0.5, 0.125, ((0, 8),))
    seq_len = draw_seq_len(jax.random.fold_in(arg_keys[6], 71), 0)
    return {"queries": queries, "keys": keys, "values": values, "out_grad": out_grad, "out_weight": out_weight, "seq_len": seq_len}


SCALE = 0.0625
CAP = 50.0

def band_block(q_rows, k_rows, v_rows, g_rows, q_pos, k_pos):
    count = q_rows.shape[0]
    span = k_rows.shape[0]
    group = HEADS // KV_HEADS
    qh = q_rows.astype(jnp.float32).reshape(count, KV_HEADS, group, HEAD_DIM)
    kh = k_rows.astype(jnp.float32).reshape(span, KV_HEADS, HEAD_DIM)
    vh = v_rows.astype(jnp.float32).reshape(span, KV_HEADS, HEAD_DIM)
    gh = g_rows.astype(jnp.float32).reshape(count, KV_HEADS, group, HEAD_DIM)
    raw = jnp.einsum('tkgd,jkd->kgtj', qh, kh) * SCALE
    capped = CAP * jnp.tanh(raw / CAP)
    allowed = (k_pos[None, :] >= 0) & (k_pos[None, :] <= q_pos[:, None]) & (k_pos[None, :] > q_pos[:, None] - WINDOW)
    expo = jnp.where(allowed, jnp.exp(capped), jnp.zeros((), jnp.float32))
    probs = expo / lax.optimization_barrier(jnp.sum(expo, axis=-1, keepdims=True))
    probs_b = probs.astype(jnp.bfloat16)
    attn = jnp.einsum('kgtj,jkd->tkgd', probs_b.astype(jnp.float32), vh).astype(jnp.bfloat16)
    delta = jnp.einsum('tkgd,tkgd->kgt', gh, attn.astype(jnp.float32))[..., None]
    dprob = jnp.einsum('tkgd,jkd->kgtj', gh, vh)
    dscore = (probs * (dprob - delta) * (1.0 - (capped / CAP) ** 2) * SCALE).astype(jnp.bfloat16)
    dscore32 = dscore.astype(jnp.float32)
    dq = jnp.einsum('kgtj,jkd->tkgd', dscore32, kh).reshape(count, -1)
    dk = jnp.einsum('kgtj,tkgd->jkd', dscore32, qh).reshape(span, -1)
    dv = jnp.einsum('kgtj,tkgd->jkd', probs_b.astype(jnp.float32), gh).reshape(span, -1)
    return (dq, dk, dv, attn.reshape(count, -1))

def reference(queries, keys, values, out_grad, out_weight, seq_len):
    seq = TOK_DEV * N_SEQ
    reach = (WINDOW + TOK_DEV - 2) // TOK_DEV
    lead = reach * TOK_DEV
    span = lead + TOK_DEV
    kv_width = KV_HEADS * HEAD_DIM
    q_list = []
    k_list = []
    v_list = []
    weight_raw = jnp.zeros((HEADS * HEAD_DIM, D_OUT), jnp.float32)
    count = jnp.zeros((), jnp.int32)
    for rep in range(N_DP):
        length = seq_len[rep]
        positions = jnp.arange(seq, dtype=jnp.int32)
        valid = positions < length
        masked = jnp.where(valid[:, None], out_grad[rep], jnp.zeros((), jnp.bfloat16))
        grad_attn = jnp.dot(masked, out_weight.T, preferred_element_type=jnp.float32).astype(jnp.bfloat16)
        blank = jnp.zeros((lead, kv_width), jnp.bfloat16)
        key_pad = jnp.concatenate([blank, keys[rep]], 0)
        val_pad = jnp.concatenate([blank, values[rep]], 0)
        rep_queries = queries[rep]

        def step(carry, block):
            dk_pad, dv_pad = carry
            first = (block * TOK_DEV).astype(jnp.int32)
            q_rows = lax.dynamic_slice_in_dim(rep_queries, first, TOK_DEV, 0)
            g_rows = lax.dynamic_slice_in_dim(grad_attn, first, TOK_DEV, 0)
            k_rows = lax.dynamic_slice_in_dim(key_pad, first, span, 0)
            v_rows = lax.dynamic_slice_in_dim(val_pad, first, span, 0)
            q_pos = first + jnp.arange(TOK_DEV, dtype=jnp.int32)
            k_pos = first - lead + jnp.arange(span, dtype=jnp.int32)
            dq, dk, dv, attn = band_block(q_rows, k_rows, v_rows, g_rows, q_pos, k_pos)
            dk_pad = lax.dynamic_update_slice_in_dim(dk_pad, lax.dynamic_slice_in_dim(dk_pad, first, span, 0) + dk, first, 0)
            dv_pad = lax.dynamic_update_slice_in_dim(dv_pad, lax.dynamic_slice_in_dim(dv_pad, first, span, 0) + dv, first, 0)
            return ((dk_pad, dv_pad), (dq, attn))
        init = (jnp.zeros((seq + lead, kv_width), jnp.float32), jnp.zeros((seq + lead, kv_width), jnp.float32))
        (dk_pad, dv_pad), (dq_blocks, attn_blocks) = lax.scan(step, init, jnp.arange(N_SEQ, dtype=jnp.int32))
        q_list.append(dq_blocks.reshape(seq, -1))
        k_list.append(dk_pad[lead:])
        v_list.append(dv_pad[lead:])
        attn_full = attn_blocks.reshape(seq, -1)
        weight_raw = weight_raw + jnp.dot(attn_full.T, masked, preferred_element_type=jnp.float32)
        count = count + jnp.sum(valid.astype(jnp.int32))
    total = count.astype(jnp.float32)
    act_scale = N_DP * seq / total
    weight_scale = lax.rsqrt(total)
    dq_all = jnp.stack(q_list) * act_scale
    dk_all = jnp.stack(k_list) * act_scale
    dv_all = jnp.stack(v_list) * act_scale
    weight_grad = weight_raw * weight_scale
    squares = jnp.sum(dq_all * dq_all) + jnp.sum(dk_all * dk_all) + jnp.sum(dv_all * dv_all) + jnp.sum(weight_grad * weight_grad)
    entries = N_DP * seq * (HEADS + 2 * KV_HEADS) * HEAD_DIM + HEADS * HEAD_DIM * D_OUT
    grad_rms = jnp.sqrt(squares / entries)
    return (dq_all.astype(jnp.bfloat16), dk_all.astype(jnp.bfloat16), dv_all.astype(jnp.bfloat16), weight_grad, grad_rms)
```

```python
import functools

import jax
import jax.numpy as jnp
from jax import lax
from jax.experimental import pallas as pl
from jax.experimental.pallas import tpu as pltpu
from jax.sharding import PartitionSpec as P

HEADS = 8
KV_HEADS = 4
HEAD_DIM = 256
D_OUT = 1792
WINDOW = 512
TOK_DEV = 256


SCALE = 0.0625
CAP = 50.0


def shifted(value, axis, steps):
    count = lax.axis_size(axis)
    initial, last = (max(0, -steps), min(count, count - steps))
    return lax.ppermute(value, axis, [(source, source + steps) for source in range(initial, last)])


def band_block(q_rows, k_rows, v_rows, g_rows, q_pos, k_pos):
    count = q_rows.shape[0]
    span = k_rows.shape[0]
    group = HEADS // KV_HEADS
    qh = q_rows.reshape(count, KV_HEADS, group, HEAD_DIM)
    kh = k_rows.reshape(span, KV_HEADS, HEAD_DIM)
    vh = v_rows.reshape(span, KV_HEADS, HEAD_DIM)
    gh = g_rows.reshape(count, KV_HEADS, group, HEAD_DIM)
    raw = jnp.einsum("tkgd,jkd->kgtj", qh, kh, preferred_element_type=jnp.float32) * SCALE
    capped = CAP * jnp.tanh(raw / CAP)
    allowed = (
        (k_pos[None, :] >= 0)
        & (k_pos[None, :] <= q_pos[:, None])
        & (k_pos[None, :] > q_pos[:, None] - WINDOW)
    )
    expo = jnp.where(allowed, jnp.exp(capped), jnp.zeros((), jnp.float32))
    probs = expo / jnp.sum(expo, axis=-1, keepdims=True)
    probs_b = probs.astype(jnp.bfloat16)
    attn = jnp.einsum("kgtj,jkd->tkgd", probs_b, vh, preferred_element_type=jnp.float32).astype(
        jnp.bfloat16
    )
    delta = jnp.einsum("tkgd,tkgd->kgt", gh, attn, preferred_element_type=jnp.float32)[..., None]
    dprob = jnp.einsum("tkgd,jkd->kgtj", gh, vh, preferred_element_type=jnp.float32)
    dscore = (probs * (dprob - delta) * (1.0 - (capped / CAP) ** 2) * SCALE).astype(jnp.bfloat16)
    dq = jnp.einsum("kgtj,jkd->tkgd", dscore, kh, preferred_element_type=jnp.float32).reshape(
        count, -1
    )
    dk = jnp.einsum("kgtj,tkgd->jkd", dscore, qh, preferred_element_type=jnp.float32).reshape(
        span, -1
    )
    dv = jnp.einsum("kgtj,tkgd->jkd", probs_b, gh, preferred_element_type=jnp.float32).reshape(
        span, -1
    )
    return (dq, dk, dv, attn.reshape(count, -1))


def shards(queries, keys, values, out_grad, out_weight, seq_len):
    q_rows = queries[0]
    k_rows = keys[0]
    v_rows = values[0]
    length = seq_len[0]
    seq_devices = lax.axis_size("seq")
    rep_devices = lax.axis_size("dp")
    start = lax.axis_index("seq") * TOK_DEV
    positions = start + jnp.arange(TOK_DEV, dtype=jnp.int32)
    valid = positions < length
    masked = jnp.where(valid[:, None], out_grad[0], jnp.zeros((), jnp.bfloat16))
    grad_attn = lax.dot_general(
        masked,
        lax.all_gather(out_weight, "seq", axis=0, tiled=True),
        (((1,), (1,)), ((), ())),
        preferred_element_type=jnp.float32,
    ).astype(jnp.bfloat16)
    reach = (WINDOW + TOK_DEV - 2) // TOK_DEV
    lead = reach * TOK_DEV
    key_parts = []
    val_parts = []
    for back in range(reach, 0, -1):
        earlier_k, earlier_v = shifted((k_rows, v_rows), "seq", back)
        key_parts.append(earlier_k)
        val_parts.append(earlier_v)
    key_block = jnp.concatenate(key_parts + [k_rows], 0)
    val_block = jnp.concatenate(val_parts + [v_rows], 0)
    k_pos = start - lead + jnp.arange(lead + TOK_DEV, dtype=jnp.int32)
    dq_raw, dk_all, dv_all, attn = band_block(
        q_rows, key_block, val_block, grad_attn, positions, k_pos
    )
    dk_raw = dk_all[lead:]
    dv_raw = dv_all[lead:]
    for back in range(1, reach + 1):
        first = (reach - back) * TOK_DEV
        later_k, later_v = (
            shifted(dk_all[first : first + TOK_DEV].astype(jnp.bfloat16), "seq", -back).astype(
                jnp.float32
            ),
            shifted(dv_all[first : first + TOK_DEV].astype(jnp.bfloat16), "seq", -back).astype(
                jnp.float32
            ),
        )
        dk_raw = dk_raw + later_k
        dv_raw = dv_raw + later_v
    width = HEADS * HEAD_DIM
    weight_raw = lax.psum_scatter(
        lax.dot_general(attn, masked, (((0,), (0,)), ((), ())), preferred_element_type=jnp.float32),
        ("seq", "dp"),
        scatter_dimension=0,
        tiled=True,
    )
    weight_sq = jnp.sum(weight_raw * weight_raw)
    own_count = jnp.clip(length - start, 0, TOK_DEV)
    slots = TOK_DEV * seq_devices * rep_devices
    entries = slots * (HEADS + 2 * KV_HEADS) * HEAD_DIM + width * D_OUT
    total = lax.psum(own_count, ("seq", "dp")).astype(jnp.float32)
    act_scale = slots / total
    weight_scale = lax.rsqrt(total)
    dq_s = dq_raw * act_scale
    dk_s = dk_raw * act_scale
    dv_s = dv_raw * act_scale
    local = (
        jnp.sum(dq_s * dq_s)
        + jnp.sum(dk_s * dk_s)
        + jnp.sum(dv_s * dv_s)
        + weight_sq * (weight_scale * weight_scale)
    )
    squares = lax.psum(local, ("seq", "dp"))
    grad_rms = jnp.sqrt(squares / entries)
    weight_grad = weight_raw * weight_scale
    weight_grad = lax.all_gather(weight_grad.astype(jnp.bfloat16), "dp", axis=0, tiled=True).astype(
        weight_grad.dtype
    )
    return (
        dq_s.astype(jnp.bfloat16)[None],
        dk_s.astype(jnp.bfloat16)[None],
        dv_s.astype(jnp.bfloat16)[None],
        weight_grad,
        grad_rms,
    )


def plain_solution(mesh):
    in_specs = (
        P("dp", "seq", None),
        P("dp", "seq", None),
        P("dp", "seq", None),
        P("dp", "seq", None),
        P("seq", None),
        P("dp"),
    )
    out_specs = (
        P("dp", "seq", None),
        P("dp", "seq", None),
        P("dp", "seq", None),
        P("seq", None),
        P(),
    )
    return jax.shard_map(shards, mesh=mesh, in_specs=in_specs, out_specs=out_specs, check_vma=False)


MESH = pl.DeviceIdType.MESH
F32, BF16 = jnp.float32, jnp.bfloat16
VMEM_LIMIT = 60 * 1024 * 1024


class Place:
    def __init__(self, n_seq):
        self.n = n_seq
        self.nz = n_seq // 2
        self.seq = lax.axis_index("seq")
        self.dp = lax.axis_index("dp")
        self.z, self.y = self.seq // 2, self.seq % 2
        self.core = self.dp % 2
        self.turn = 1 - 2 * self.core
        self.pos = self.z + self.y * (n_seq - 1 - 2 * self.z)

    def ring(self, offset):
        p = (self.pos + self.turn * offset + 4 * self.n) % self.n
        far = p // self.nz
        z = p + far * (self.n - 1 - 2 * p)
        return 2 * z + far

    def dp_flip(self, k):
        if k == 1:
            return self.dp + 1 - 2 * self.core
        if k == 2:
            return (self.dp + 2) % 4
        return 3 - self.dp

    def y_flip(self):
        return self.seq + 1 - 2 * self.y


def remote(src, dst, send, recv, seq, dp):
    return pltpu.make_async_remote_copy(
        src_ref=src, dst_ref=dst, send_sem=send, recv_sem=recv, device_id=(seq, dp), device_id_type=MESH
    )


def meet(peers):
    barrier = pltpu.get_barrier_semaphore()
    for seq, dp in peers:
        pl.semaphore_signal(barrier, inc=1, device_id=(seq, dp), device_id_type=MESH)
    pl.semaphore_wait(barrier, len(peers))


def rows_at(first, count):
    return pl.ds(pl.multiple_of(first, count), count)


def gather_kernel(n_seq, w_ref, k_ref, v_ref, len_ref, w_full, k_halo, v_halo, total_ref,
                  lens, zeros, ring_s, ring_r, x_s, x_r, c_s, c_r, cx_s, cx_r,
                  z_s, z_r, y_s, y_r, l_s, l_r, own_sem):
    at = Place(n_seq)
    seq, dp, z, y, nz = at.seq, at.dp, at.z, at.y, at.nz
    part = w_ref.shape[0]
    quarter = part // 4
    tok = k_ref.shape[0]
    meet([(at.ring(1), dp), (at.ring(-1), dp), (at.y_flip(), dp)] + [(seq, at.dp_flip(k)) for k in (1, 2, 3)])

    def piece(owner, q):
        return w_full.at[rows_at(owner * part + q * quarter, quarter)]

    steps = n_seq - 1

    def ring_copy(t):
        owner = at.ring(-t)
        src = w_ref.at[rows_at(dp * quarter, quarter)] if t == 0 else piece(owner, dp)
        return remote(src, piece(owner, dp), ring_s.at[t], ring_r.at[t], at.ring(1), dp)

    def x_copy(t):
        spot = piece(at.ring(-t - 1), dp)
        return remote(spot, spot, x_s.at[t], x_r.at[t], seq, at.dp_flip(2))

    def c_copy(t):
        spot = piece(at.ring(-t - 1), dp)
        return remote(spot, spot, c_s.at[t], c_r.at[t], seq, at.dp_flip(1))

    def cx_copy(t):
        spot = piece(at.ring(-t - 1), at.dp_flip(2))
        return remote(spot, spot, cx_s.at[t], cx_r.at[t], seq, at.dp_flip(1))

    blocks, halos = (k_ref, v_ref), (k_halo, v_halo)
    up = jnp.minimum(seq + 2, n_seq - 1 - (1 - y))

    def z_copy(i):
        return remote(blocks[i], halos[i].at[pl.ds(0, tok)], z_s.at[i], z_r.at[i], up, dp)

    def y_copy(i, relay):
        src = halos[i].at[pl.ds(0, tok)] if relay else blocks[i]
        return remote(src, halos[i].at[pl.ds(tok, tok)], y_s.at[i], y_r.at[i], at.y_flip(), dp)

    ring = [ring_copy(t) for t in range(steps)]
    xc = [x_copy(t) for t in range(steps)]
    cc = [c_copy(t) for t in range(steps)]
    cx = [cx_copy(t) for t in range(steps)]

    len_copies = [remote(len_ref, lens.at[k - 1], l_s.at[k - 1], l_r.at[k - 1], seq, at.dp_flip(k)) for k in (1, 2, 3)]
    ring[0].start()
    for c in len_copies:
        c.start()

    @pl.when(z < nz - 1)
    def _():
        z_copy(0).start()

    @pl.when(y == 0)
    def _():
        y_copy(0, False).start()
        y_copy(1, False).start()

    own = pltpu.make_async_copy(w_ref, w_full.at[rows_at(seq * part, part)], own_sem.at[0])
    own.start()

    @pl.when(z == 0)
    def _():
        zeros[...] = jnp.zeros_like(zeros)
        for i in range(2):
            c = pltpu.make_async_copy(zeros, halos[i].at[pl.ds(0, tok)], own_sem.at[1 + i])
            c.start()
            c.wait()

        @pl.when(y == 0)
        def _():
            for i in range(2):
                c = pltpu.make_async_copy(zeros, halos[i].at[pl.ds(tok, tok)], own_sem.at[1 + i])
                c.start()
                c.wait()

    def relay(i):
        @pl.when(z > 0)
        def _():
            z_copy(i).wait_recv()

            @pl.when(y == 1)
            def _():
                y_copy(i, True).start()

    for t in range(steps):
        ring[t].wait_recv()
        if t + 1 < steps:
            ring[t + 1].start()
        xc[t].start()
        cc[t].start()
        if t > 0:
            xc[t - 1].wait_recv()
            cx[t - 1].start()
        if t == 2:
            @pl.when(z < nz - 1)
            def _():
                z_copy(1).start()
        if t == 3:
            relay(0)
    relay(1)
    xc[steps - 1].wait_recv()
    cx[steps - 1].start()
    for c in len_copies:
        c.wait()
    total_ref[...] = len_ref[...] + lens[0] + lens[1] + lens[2]
    for t in range(steps):
        cc[t].wait_recv()
        cx[t].wait_recv()

    @pl.when((y == 1) | (z > 0))
    def _():
        for i in range(2):
            y_copy(i, False).wait_recv()

    @pl.when((y == 0) | (z > 0))
    def _():
        for i in range(2):
            y_copy(i, False).wait_send()

    @pl.when(z < nz - 1)
    def _():
        for i in range(2):
            z_copy(i).wait_send()

    own.wait()
    for t in range(steps):
        ring[t].wait_send()
        xc[t].wait_send()
        cc[t].wait_send()
        cx[t].wait_send()


def dot_t(a, b):
    return lax.dot_general(a, b, (((1,), (1,)), ((), ())), preferred_element_type=F32)


def dot_0(a, b):
    return lax.dot_general(a, b, (((0,), (0,)), ((), ())), preferred_element_type=F32)


def dot_n(a, b):
    return lax.dot_general(a, b, (((1,), (0,)), ((), ())), preferred_element_type=F32)


def tile_sum(x):
    r, c = x.shape
    s = jnp.sum(x.reshape(r // 8, 8, c), axis=0)
    out = s[:, 0:128]
    for j in range(1, c // 128):
        out = out + s[:, j * 128 : (j + 1) * 128]
    return out


def attend_kernel(group, info_ref, act_ref, q_ref, k_ref, v_ref, kh_ref, vh_ref, g_ref, w_ref,
                  dq_ref, dk_ref, dv_ref, dkh_ref, dvh_ref, wg_ref, sq_ref, masked_ref):
    start, length = info_ref[0], info_ref[1]
    tok, dim = k_ref.shape
    lead = kh_ref.shape[0]
    span = lead + tok
    act = act_ref[0, 0]

    @pl.when(pl.program_id(0) == 0)
    def _():
        row = start + lax.broadcasted_iota(jnp.int32, (tok, 1), 0)
        masked_ref[...] = jnp.where(row < length, g_ref[...].astype(F32), 0.0).astype(BF16)
        sq_ref[...] = jnp.zeros_like(sq_ref)

    masked = masked_ref[...]
    kc = jnp.concatenate([kh_ref[...], k_ref[...]], 0)
    vc = jnp.concatenate([vh_ref[...], v_ref[...]], 0)
    qi = lax.broadcasted_iota(jnp.int32, (tok, span), 0)
    kj = lax.broadcasted_iota(jnp.int32, (tok, span), 1) - lead
    allowed = (kj <= qi) & (kj > qi - WINDOW) & (kj + start >= 0)
    dk = dv = None
    for h in range(group):
        cols = slice(h * dim, (h + 1) * dim)
        qh = q_ref[:, cols]
        gh = dot_t(masked, w_ref[cols, :]).astype(BF16)
        t = jnp.tanh(dot_t(qh, kc) * (SCALE / CAP))
        e = jnp.where(allowed, jnp.exp(CAP * t), 0.0)
        p = e * (1.0 / jnp.sum(e, axis=-1, keepdims=True))
        pb = p.astype(BF16)
        attn = dot_n(pb, vc).astype(BF16)
        delta = jnp.sum(gh.astype(F32) * attn.astype(F32), axis=-1, keepdims=True)
        ds = (p * (dot_t(gh, vc) - delta) * ((1.0 - t * t) * SCALE)).astype(BF16)
        dq = dot_n(ds, kc) * act
        dq_ref[:, cols] = dq.astype(BF16)
        sq_ref[...] += tile_sum(dq * dq)
        dkh = dot_0(ds, qh)
        dvh = dot_0(pb, gh)
        dk = dkh if dk is None else dk + dkh
        dv = dvh if dv is None else dv + dvh
        wg_ref[cols, :] = dot_0(attn, masked).astype(BF16)
    dk_ref[...] = dk[lead:]
    dv_ref[...] = dv[lead:]
    dkh_ref[...] = dk[:lead].astype(BF16)
    dvh_ref[...] = dv[:lead].astype(BF16)


def reduce_kernel(n_seq, entries, wg_ref, dk_ref, dv_ref, dkh_ref, dvh_ref, sq_ref, total_ref,
                  kg_ref, vg_ref, wgrad_ref, rms_ref,
                  cbuf, xsend, xbuf, rsend, rbuf, gown, gbuf, ybuf, zbuf, zsend, s_own, s_in, s_mid, s_all,
                  c_s, c_r, x_s, x_r, r_s, r_r, g_s, g_r, y_s, y_r, z_s, z_r, a_s, a_r, b_s, b_r):
    at = Place(n_seq)
    seq, dp, z, y, nz = at.seq, at.dp, at.z, at.y, at.nz
    part = wg_ref.shape[0] // n_seq
    half, quarter = part // 2, part // 4
    tok = dk_ref.shape[0]
    x = dp // 2
    meet(
        [(at.ring(1), dp), (at.ring(-1), dp), (at.y_flip(), dp)]
        + [(seq, at.dp_flip(k)) for k in (1, 2, 3)]
        + [((seq + k) % n_seq, dp) for k in range(1, n_seq)]
    )
    def quarter_row(d):
        return (d % 2) * half + (d // 2) * quarter

    def c_copy(u):
        owner = at.ring(u + 1)
        src = wg_ref.at[rows_at(owner * part + (1 - at.core) * half, half)]
        return remote(src, cbuf.at[u], c_s.at[u], c_r.at[u], seq, at.dp_flip(1))

    cc = [c_copy(u) for u in range(n_seq)]
    xc = [remote(xsend.at[u], xbuf.at[u], x_s.at[u], x_r.at[u], seq, at.dp_flip(2)) for u in range(n_seq)]
    rc = [remote(rsend.at[u], rbuf.at[u], r_s.at[u], r_r.at[u], at.ring(1), dp) for u in range(n_seq - 1)]
    halos = (dkh_ref, dvh_ref)
    down = jnp.maximum(seq - 2, y)

    def y_copy(i):
        return remote(halos[i].at[pl.ds(tok, tok)], ybuf.at[i], y_s.at[i], y_r.at[i], at.y_flip(), dp)

    def z_copy(i, summed):
        src = zsend.at[i] if summed else halos[i].at[pl.ds(0, tok)]
        return remote(src, zbuf.at[i], z_s.at[i], z_r.at[i], down, dp)

    for u in range(n_seq):
        cc[u].start()

    @pl.when((y == 1) | (z > 0))
    def _():
        for i in range(2):
            y_copy(i).start()

    @pl.when((y == 0) & (z > 0))
    def _():
        for i in range(2):
            z_copy(i, False).start()

    for u in range(n_seq):
        cc[u].wait_recv()
        first = at.ring(-u - 1) * part + at.core * half + (1 - x) * quarter
        mine = wg_ref[rows_at(first, quarter), :].astype(F32)
        theirs = cbuf[u, rows_at((1 - x) * quarter, quarter), :].astype(F32)
        xsend[u] = (mine + theirs).astype(BF16)
        xc[u].start()

    def chunk(u):
        first = at.ring(-u - 1) * part + at.core * half + x * quarter
        acc = wg_ref[rows_at(first, quarter), :].astype(F32)
        acc = acc + cbuf[u, rows_at(x * quarter, quarter), :].astype(F32)
        xc[u].wait_recv()
        acc = acc + xbuf[u].astype(F32)
        if u > 0:
            rc[u - 1].wait_recv()
            acc = acc + rbuf[u - 1].astype(F32)
        return acc

    def relay(i):
        @pl.when((y == 0) | (z > 0))
        def _():
            y_copy(i).wait_recv()

        @pl.when((y == 1) & (z > 0))
        def _():
            zsend[i] = (halos[i][0:tok, :].astype(F32) + ybuf[i].astype(F32)).astype(BF16)
            z_copy(i, True).start()

    for u in range(n_seq - 1):
        rsend[u] = chunk(u).astype(BF16)
        rc[u].start()
        if u == 1:
            relay(0)
        if u == 3:
            relay(1)

    total = total_ref[0:1, 0:1]
    act = (tok * n_seq * 4) / total
    wscale = lax.rsqrt(total)
    grads = []
    square = sq_ref[...]
    for i, (own, out) in enumerate(((dk_ref, kg_ref), (dv_ref, vg_ref))):
        @pl.when(z < nz - 1)
        def _():
            z_copy(i, False).wait_recv()

        val = own[...]
        val = val + jnp.where(y == 0, ybuf[i].astype(F32), 0.0)
        val = val + jnp.where(z < nz - 1, zbuf[i].astype(F32), 0.0)
        val = val * act
        out[...] = val.astype(BF16)
        square = square + tile_sum(val * val)

    raw = chunk(n_seq - 1)
    gown[...] = raw.astype(BF16)
    gc = [remote(gown, gbuf.at[k - 1], g_s.at[k - 1], g_r.at[k - 1], seq, at.dp_flip(k)) for k in (1, 2, 3)]
    scaled = raw * wscale
    s_own[...] = square + tile_sum(scaled * scaled)
    ac = [remote(s_own, s_in.at[k - 1], a_s.at[k - 1], a_r.at[k - 1], seq, at.dp_flip(k)) for k in (1, 2, 3)]
    for c in ac:
        c.start()
    for c in gc:
        c.start()
    for c in ac:
        c.wait_recv()
    s_mid[...] = (s_own[...] + s_in[1]) + (s_in[0] + s_in[2])
    bc = [
        remote(s_mid, s_all.at[k - 1], b_s.at[k - 1], b_r.at[k - 1], (seq + k) % n_seq, dp)
        for k in range(1, n_seq)
    ]
    for c in bc:
        c.start()
    wgrad_ref[rows_at(quarter_row(dp), quarter), :] = gown[...].astype(F32) * wscale
    for k in (1, 2, 3):
        gc[k - 1].wait_recv()
        wgrad_ref[rows_at(quarter_row(at.dp_flip(k)), quarter), :] = gbuf[k - 1].astype(F32) * wscale
    for c in bc:
        c.wait_recv()
    final = s_mid[...]
    for k in range(n_seq - 1):
        final = final + s_all[k]
    whole = jnp.sum(jnp.sum(final, axis=1, keepdims=True), axis=0, keepdims=True)
    rms_ref[...] = jnp.broadcast_to(jnp.sqrt(whole / entries), rms_ref.shape)

    for c in cc + xc + rc + gc + ac + bc:
        c.wait_send()

    @pl.when((y == 1) | (z > 0))
    def _():
        for i in range(2):
            y_copy(i).wait_send()

    @pl.when(z > 0)
    def _():
        for i in range(2):
            z_copy(i, False).wait_send()


ANY = pl.BlockSpec(memory_space=pl.ANY)
VM = pl.BlockSpec(memory_space=pltpu.VMEM)
DMA = pltpu.SemaphoreType.DMA


def fast_shards(n_seq, queries, keys, values, out_grad, out_weight, seq_len):
    q, k, v, g = queries[0], keys[0], values[0], out_grad[0]
    tok, kv_width = k.shape
    part, d_out = out_weight.shape
    width = part * n_seq
    dim, group = HEAD_DIM, HEADS // KV_HEADS
    lead = 2 * tok
    steps = n_seq - 1
    sds = jax.ShapeDtypeStruct
    length = jnp.clip(seq_len[0], 0, tok * n_seq)
    len_tile = jnp.full((8, 128), length.astype(F32), F32)
    w_full, k_halo, v_halo, total = pl.pallas_call(
        functools.partial(gather_kernel, n_seq),
        out_shape=(sds((width, d_out), BF16), sds((lead, kv_width), BF16), sds((lead, kv_width), BF16), sds((8, 128), F32)),
        in_specs=[VM] * 4,
        out_specs=(ANY, ANY, ANY, VM),
        scratch_shapes=[pltpu.VMEM((3, 8, 128), F32), pltpu.VMEM((tok, kv_width), BF16)]
        + [DMA((steps,))] * 8 + [DMA((2,))] * 4 + [DMA((3,))] * 3,
        compiler_params=pltpu.CompilerParams(collective_id=0, has_side_effects=True, vmem_limit_bytes=VMEM_LIMIT // 2),
    )(out_weight, k, v, len_tile)
    start = lax.axis_index("seq").astype(jnp.int32) * tok
    info = jnp.stack([start, seq_len[0]])
    act = (tok * n_seq * 4) / total[0:1, 0:1]
    smem = pl.BlockSpec(memory_space=pltpu.SMEM)

    def col(rows, cols):
        return pl.BlockSpec((rows, cols), lambda i: (0, i))

    dq, dk, dv, dkh, dvh, wg, sq = pl.pallas_call(
        functools.partial(attend_kernel, group),
        grid=(KV_HEADS,),
        out_shape=(
            sds((tok, width), BF16), sds((tok, kv_width), F32), sds((tok, kv_width), F32),
            sds((lead, kv_width), BF16), sds((lead, kv_width), BF16), sds((width, d_out), BF16), sds((8, 128), F32),
        ),
        in_specs=[
            smem, smem, col(tok, group * dim), col(tok, dim), col(tok, dim), col(lead, dim), col(lead, dim),
            pl.BlockSpec((tok, d_out), lambda i: (0, 0)), pl.BlockSpec((group * dim, d_out), lambda i: (i, 0)),
        ],
        out_specs=(
            col(tok, group * dim), col(tok, dim), col(tok, dim), col(lead, dim), col(lead, dim),
            pl.BlockSpec((group * dim, d_out), lambda i: (i, 0)), pl.BlockSpec((8, 128), lambda i: (0, 0)),
        ),
        scratch_shapes=[pltpu.VMEM((tok, d_out), BF16)],
        compiler_params=pltpu.CompilerParams(dimension_semantics=("arbitrary",), vmem_limit_bytes=VMEM_LIMIT),
    )(info, act, q, k, v, k_halo, v_halo, g, w_full)
    entries = tok * n_seq * 4 * (HEADS + 2 * KV_HEADS) * HEAD_DIM + width * d_out
    quarter = part // 4
    kg, vg, wgrad, rms = pl.pallas_call(
        functools.partial(reduce_kernel, n_seq, float(entries)),
        out_shape=(sds((tok, kv_width), BF16), sds((tok, kv_width), BF16), sds((part, d_out), F32), sds((8, 128), F32)),
        in_specs=[VM] * 7,
        out_specs=(VM,) * 4,
        scratch_shapes=[
            pltpu.VMEM((n_seq, part // 2, d_out), BF16),
            pltpu.VMEM((n_seq, quarter, d_out), BF16),
            pltpu.VMEM((n_seq, quarter, d_out), BF16),
            pltpu.VMEM((steps, quarter, d_out), BF16),
            pltpu.VMEM((steps, quarter, d_out), BF16),
            pltpu.VMEM((quarter, d_out), BF16),
            pltpu.VMEM((3, quarter, d_out), BF16),
            pltpu.VMEM((2, tok, kv_width), BF16),
            pltpu.VMEM((2, tok, kv_width), BF16),
            pltpu.VMEM((2, tok, kv_width), BF16),
            pltpu.VMEM((8, 128), F32),
            pltpu.VMEM((3, 8, 128), F32),
            pltpu.VMEM((8, 128), F32),
            pltpu.VMEM((steps, 8, 128), F32),
            DMA((n_seq,)), DMA((n_seq,)), DMA((n_seq,)), DMA((n_seq,)), DMA((steps,)), DMA((steps,)),
            DMA((3,)), DMA((3,)), DMA((2,)), DMA((2,)), DMA((2,)), DMA((2,)),
            DMA((3,)), DMA((3,)), DMA((steps,)), DMA((steps,)),
        ],
        compiler_params=pltpu.CompilerParams(collective_id=1, has_side_effects=True, vmem_limit_bytes=VMEM_LIMIT),
    )(wg, dk, dv, dkh, dvh, sq, total)
    return dq[None], kg[None], vg[None], wgrad, rms[0, 0]


def solution(mesh):
    n_seq, n_dp = mesh.shape["seq"], mesh.shape["dp"]
    if n_seq != HEADS or n_dp != 4:
        return plain_solution(mesh)
    row = P("dp", "seq", None)
    return jax.shard_map(
        functools.partial(fast_shards, n_seq),
        mesh=mesh,
        in_specs=(row, row, row, row, P("seq", None), P("dp")),
        out_specs=(row, row, row, P("seq", None), P()),
        check_vma=False,
    )
```

```python
import functools

import jax
import jax.numpy as jnp
from jax import lax
from jax.experimental import pallas as pl
from jax.experimental.pallas import tpu as pltpu
from jax.sharding import PartitionSpec as P

HEADS = 8
KV_HEADS = 4
HEAD_DIM = 256
D_OUT = 1792
WINDOW = 512
TOK_DEV = 256


SCALE = 0.0625
CAP = 50.0


def shifted(value, axis, steps):
    count = lax.axis_size(axis)
    initial, last = (max(0, -steps), min(count, count - steps))
    return lax.ppermute(value, axis, [(source, source + steps) for source in range(initial, last)])


def band_block(q_rows, k_rows, v_rows, g_rows, q_pos, k_pos):
    count = q_rows.shape[0]
    span = k_rows.shape[0]
    group = HEADS // KV_HEADS
    qh = q_rows.reshape(count, KV_HEADS, group, HEAD_DIM)
    kh = k_rows.reshape(span, KV_HEADS, HEAD_DIM)
    vh = v_rows.reshape(span, KV_HEADS, HEAD_DIM)
    gh = g_rows.reshape(count, KV_HEADS, group, HEAD_DIM)
    raw = jnp.einsum("tkgd,jkd->kgtj", qh, kh, preferred_element_type=jnp.float32) * SCALE
    capped = CAP * jnp.tanh(raw / CAP)
    allowed = (
        (k_pos[None, :] >= 0)
        & (k_pos[None, :] <= q_pos[:, None])
        & (k_pos[None, :] > q_pos[:, None] - WINDOW)
    )
    expo = jnp.where(allowed, jnp.exp(capped), jnp.zeros((), jnp.float32))
    probs = expo / jnp.sum(expo, axis=-1, keepdims=True)
    probs_b = probs.astype(jnp.bfloat16)
    attn = jnp.einsum("kgtj,jkd->tkgd", probs_b, vh, preferred_element_type=jnp.float32).astype(
        jnp.bfloat16
    )
    delta = jnp.einsum("tkgd,tkgd->kgt", gh, attn, preferred_element_type=jnp.float32)[..., None]
    dprob = jnp.einsum("tkgd,jkd->kgtj", gh, vh, preferred_element_type=jnp.float32)
    dscore = (probs * (dprob - delta) * (1.0 - (capped / CAP) ** 2) * SCALE).astype(jnp.bfloat16)
    dq = jnp.einsum("kgtj,jkd->tkgd", dscore, kh, preferred_element_type=jnp.float32).reshape(
        count, -1
    )
    dk = jnp.einsum("kgtj,tkgd->jkd", dscore, qh, preferred_element_type=jnp.float32).reshape(
        span, -1
    )
    dv = jnp.einsum("kgtj,tkgd->jkd", probs_b, gh, preferred_element_type=jnp.float32).reshape(
        span, -1
    )
    return (dq, dk, dv, attn.reshape(count, -1))


def shards(queries, keys, values, out_grad, out_weight, seq_len):
    q_rows = queries[0]
    k_rows = keys[0]
    v_rows = values[0]
    length = seq_len[0]
    seq_devices = lax.axis_size("seq")
    rep_devices = lax.axis_size("dp")
    start = lax.axis_index("seq") * TOK_DEV
    positions = start + jnp.arange(TOK_DEV, dtype=jnp.int32)
    valid = positions < length
    masked = jnp.where(valid[:, None], out_grad[0], jnp.zeros((), jnp.bfloat16))
    grad_attn = lax.dot_general(
        masked,
        lax.all_gather(out_weight, "seq", axis=0, tiled=True),
        (((1,), (1,)), ((), ())),
        preferred_element_type=jnp.float32,
    ).astype(jnp.bfloat16)
    reach = (WINDOW + TOK_DEV - 2) // TOK_DEV
    lead = reach * TOK_DEV
    key_parts = []
    val_parts = []
    for back in range(reach, 0, -1):
        earlier_k, earlier_v = shifted((k_rows, v_rows), "seq", back)
        key_parts.append(earlier_k)
        val_parts.append(earlier_v)
    key_block = jnp.concatenate(key_parts + [k_rows], 0)
    val_block = jnp.concatenate(val_parts + [v_rows], 0)
    k_pos = start - lead + jnp.arange(lead + TOK_DEV, dtype=jnp.int32)
    dq_raw, dk_all, dv_all, attn = band_block(
        q_rows, key_block, val_block, grad_attn, positions, k_pos
    )
    dk_raw = dk_all[lead:]
    dv_raw = dv_all[lead:]
    for back in range(1, reach + 1):
        first = (reach - back) * TOK_DEV
        later_k, later_v = (
            shifted(dk_all[first : first + TOK_DEV].astype(jnp.bfloat16), "seq", -back).astype(
                jnp.float32
            ),
            shifted(dv_all[first : first + TOK_DEV].astype(jnp.bfloat16), "seq", -back).astype(
                jnp.float32
            ),
        )
        dk_raw = dk_raw + later_k
        dv_raw = dv_raw + later_v
    width = HEADS * HEAD_DIM
    weight_raw = lax.psum_scatter(
        lax.dot_general(attn, masked, (((0,), (0,)), ((), ())), preferred_element_type=jnp.float32),
        ("seq", "dp"),
        scatter_dimension=0,
        tiled=True,
    )
    weight_sq = jnp.sum(weight_raw * weight_raw)
    own_count = jnp.clip(length - start, 0, TOK_DEV)
    slots = TOK_DEV * seq_devices * rep_devices
    entries = slots * (HEADS + 2 * KV_HEADS) * HEAD_DIM + width * D_OUT
    total = lax.psum(own_count, ("seq", "dp")).astype(jnp.float32)
    act_scale = slots / total
    weight_scale = lax.rsqrt(total)
    dq_s = dq_raw * act_scale
    dk_s = dk_raw * act_scale
    dv_s = dv_raw * act_scale
    local = (
        jnp.sum(dq_s * dq_s)
        + jnp.sum(dk_s * dk_s)
        + jnp.sum(dv_s * dv_s)
        + weight_sq * (weight_scale * weight_scale)
    )
    squares = lax.psum(local, ("seq", "dp"))
    grad_rms = jnp.sqrt(squares / entries)
    weight_grad = weight_raw * weight_scale
    weight_grad = lax.all_gather(weight_grad.astype(jnp.bfloat16), "dp", axis=0, tiled=True).astype(
        weight_grad.dtype
    )
    return (
        dq_s.astype(jnp.bfloat16)[None],
        dk_s.astype(jnp.bfloat16)[None],
        dv_s.astype(jnp.bfloat16)[None],
        weight_grad,
        grad_rms,
    )


def plain_solution(mesh):
    in_specs = (
        P("dp", "seq", None),
        P("dp", "seq", None),
        P("dp", "seq", None),
        P("dp", "seq", None),
        P("seq", None),
        P("dp"),
    )
    out_specs = (
        P("dp", "seq", None),
        P("dp", "seq", None),
        P("dp", "seq", None),
        P("seq", None),
        P(),
    )
    return jax.shard_map(shards, mesh=mesh, in_specs=in_specs, out_specs=out_specs, check_vma=False)


MESH = pl.DeviceIdType.MESH
F32, BF16 = jnp.float32, jnp.bfloat16
VMEM_LIMIT = 67043328


class Place:
    def __init__(self, n_seq):
        self.n = n_seq
        self.nz = n_seq // 2
        self.seq = lax.axis_index("seq")
        self.dp = lax.axis_index("dp")
        self.z, self.y = self.seq // 2, self.seq % 2
        self.core = self.dp % 2
        self.turn = 1 - 2 * self.core
        self.pos = self.z + self.y * (n_seq - 1 - 2 * self.z)

    def ring(self, offset):
        p = (self.pos + self.turn * offset + 4 * self.n) % self.n
        far = p // self.nz
        z = p + far * (self.n - 1 - 2 * p)
        return 2 * z + far

    def dp_flip(self, k):
        if k == 1:
            return self.dp + 1 - 2 * self.core
        if k == 2:
            return (self.dp + 2) % 4
        return 3 - self.dp

    def y_flip(self):
        return self.seq + 1 - 2 * self.y


def remote(src, dst, send, recv, seq, dp):
    return pltpu.make_async_remote_copy(
        src_ref=src, dst_ref=dst, send_sem=send, recv_sem=recv, device_id=(seq, dp), device_id_type=MESH
    )


def meet(peers):
    barrier = pltpu.get_barrier_semaphore()
    for seq, dp in peers:
        pl.semaphore_signal(barrier, inc=1, device_id=(seq, dp), device_id_type=MESH)
    pl.semaphore_wait(barrier, len(peers))


def rows_at(first, count):
    return pl.ds(pl.multiple_of(first, count), count)


def gather_kernel(n_seq, w_ref, k_ref, v_ref, len_ref, w_full, k_halo, v_halo, total_ref,
                  lens, zeros, ring_s, ring_r, x_s, x_r, c_s, c_r, cx_s, cx_r,
                  z_s, z_r, y_s, y_r, l_s, l_r, own_sem):
    at = Place(n_seq)
    seq, dp, z, y, nz = at.seq, at.dp, at.z, at.y, at.nz
    part = w_ref.shape[0]
    quarter = part // 4
    tok = k_ref.shape[0]
    meet([(at.ring(1), dp), (at.ring(-1), dp), (at.y_flip(), dp)] + [(seq, at.dp_flip(k)) for k in (1, 2, 3)])

    def piece(owner, q):
        return w_full.at[rows_at(owner * part + q * quarter, quarter)]

    steps = n_seq - 1

    def ring_copy(t):
        owner = at.ring(-t)
        src = w_ref.at[rows_at(dp * quarter, quarter)] if t == 0 else piece(owner, dp)
        return remote(src, piece(owner, dp), ring_s.at[t], ring_r.at[t], at.ring(1), dp)

    def x_copy(t):
        spot = piece(at.ring(-t - 1), dp)
        return remote(spot, spot, x_s.at[t], x_r.at[t], seq, at.dp_flip(2))

    def c_copy(t):
        spot = piece(at.ring(-t - 1), dp)
        return remote(spot, spot, c_s.at[t], c_r.at[t], seq, at.dp_flip(1))

    def cx_copy(t):
        spot = piece(at.ring(-t - 1), at.dp_flip(2))
        return remote(spot, spot, cx_s.at[t], cx_r.at[t], seq, at.dp_flip(1))

    blocks, halos = (k_ref, v_ref), (k_halo, v_halo)
    up = jnp.minimum(seq + 2, n_seq - 1 - (1 - y))

    def z_copy(i):
        return remote(blocks[i], halos[i].at[pl.ds(0, tok)], z_s.at[i], z_r.at[i], up, dp)

    def y_copy(i, relay):
        src = halos[i].at[pl.ds(0, tok)] if relay else blocks[i]
        return remote(src, halos[i].at[pl.ds(tok, tok)], y_s.at[i], y_r.at[i], at.y_flip(), dp)

    ring = [ring_copy(t) for t in range(steps)]
    xc = [x_copy(t) for t in range(steps)]
    cc = [c_copy(t) for t in range(steps)]
    cx = [cx_copy(t) for t in range(steps)]

    len_copies = [remote(len_ref, lens.at[k - 1], l_s.at[k - 1], l_r.at[k - 1], seq, at.dp_flip(k)) for k in (1, 2, 3)]
    ring[0].start()
    for c in len_copies:
        c.start()

    @pl.when(z < nz - 1)
    def _():
        z_copy(0).start()

    @pl.when(y == 0)
    def _():
        y_copy(0, False).start()
        y_copy(1, False).start()

    own = pltpu.make_async_copy(w_ref, w_full.at[rows_at(seq * part, part)], own_sem.at[0])
    own.start()

    @pl.when(z == 0)
    def _():
        zeros[...] = jnp.zeros_like(zeros)
        for i in range(2):
            c = pltpu.make_async_copy(zeros, halos[i].at[pl.ds(0, tok)], own_sem.at[1 + i])
            c.start()
            c.wait()

        @pl.when(y == 0)
        def _():
            for i in range(2):
                c = pltpu.make_async_copy(zeros, halos[i].at[pl.ds(tok, tok)], own_sem.at[1 + i])
                c.start()
                c.wait()

    def relay(i):
        @pl.when(z > 0)
        def _():
            z_copy(i).wait_recv()

            @pl.when(y == 1)
            def _():
                y_copy(i, True).start()

    for t in range(steps):
        ring[t].wait_recv()
        if t + 1 < steps:
            ring[t + 1].start()
        xc[t].start()
        cc[t].start()
        if t > 0:
            xc[t - 1].wait_recv()
            cx[t - 1].start()
        if t == 2:
            @pl.when(z < nz - 1)
            def _():
                z_copy(1).start()
        if t == 3:
            relay(0)
    relay(1)
    xc[steps - 1].wait_recv()
    cx[steps - 1].start()
    for c in len_copies:
        c.wait()
    total_ref[...] = len_ref[...] + lens[0] + lens[1] + lens[2]
    for t in range(steps):
        cc[t].wait_recv()
        cx[t].wait_recv()

    @pl.when((y == 1) | (z > 0))
    def _():
        for i in range(2):
            y_copy(i, False).wait_recv()

    @pl.when((y == 0) | (z > 0))
    def _():
        for i in range(2):
            y_copy(i, False).wait_send()

    @pl.when(z < nz - 1)
    def _():
        for i in range(2):
            z_copy(i).wait_send()

    own.wait()
    for t in range(steps):
        ring[t].wait_send()
        xc[t].wait_send()
        cc[t].wait_send()
        cx[t].wait_send()


def dot_t(a, b):
    return lax.dot_general(a, b, (((1,), (1,)), ((), ())), preferred_element_type=F32)


def dot_0(a, b):
    return lax.dot_general(a, b, (((0,), (0,)), ((), ())), preferred_element_type=F32)


def dot_n(a, b):
    return lax.dot_general(a, b, (((1,), (0,)), ((), ())), preferred_element_type=F32)


def tile_sum(x):
    r, c = x.shape
    s = jnp.sum(x.reshape(r // 8, 8, c), axis=0)
    out = s[:, 0:128]
    for j in range(1, c // 128):
        out = out + s[:, j * 128 : (j + 1) * 128]
    return out


def attend_kernel(group, info_ref, act_ref, q_ref, k_ref, v_ref, kh_ref, vh_ref, g_ref, w_ref,
                  dq_ref, dk_ref, dv_ref, dkh_ref, dvh_ref, wg_ref, sq_ref, masked_ref):
    start, length = info_ref[0], info_ref[1]
    tok, dim = k_ref.shape
    lead = kh_ref.shape[0]
    span = lead + tok
    act = act_ref[0, 0]

    @pl.when(pl.program_id(0) == 0)
    def _():
        row = start + lax.broadcasted_iota(jnp.int32, (tok, 1), 0)
        masked_ref[...] = jnp.where(row < length, g_ref[...].astype(F32), 0.0).astype(BF16)
        sq_ref[...] = jnp.zeros_like(sq_ref)

    masked = masked_ref[...]
    kc = jnp.concatenate([kh_ref[...], k_ref[...]], 0)
    vc = jnp.concatenate([vh_ref[...], v_ref[...]], 0)
    qi = lax.broadcasted_iota(jnp.int32, (tok, span), 0)
    kj = lax.broadcasted_iota(jnp.int32, (tok, span), 1) - lead
    allowed = (kj <= qi) & (kj > qi - WINDOW) & (kj + start >= 0)
    dk = dv = None
    for h in range(group):
        cols = slice(h * dim, (h + 1) * dim)
        qh = q_ref[:, cols]
        gh = dot_t(masked, w_ref[cols, :]).astype(BF16)
        t = jnp.tanh(dot_t(qh, kc) * (SCALE / CAP))
        e = jnp.where(allowed, jnp.exp(CAP * t), 0.0)
        p = e * (1.0 / jnp.sum(e, axis=-1, keepdims=True))
        pb = p.astype(BF16)
        attn = dot_n(pb, vc).astype(BF16)
        delta = jnp.sum(gh.astype(F32) * attn.astype(F32), axis=-1, keepdims=True)
        ds = (p * (dot_t(gh, vc) - delta) * ((1.0 - t * t) * SCALE)).astype(BF16)
        dq = dot_n(ds, kc) * act
        dq_ref[:, cols] = dq.astype(BF16)
        sq_ref[...] += tile_sum(dq * dq)
        dkh = dot_0(ds, qh)
        dvh = dot_0(pb, gh)
        dk = dkh if dk is None else dk + dkh
        dv = dvh if dv is None else dv + dvh
        wg_ref[cols, :] = dot_0(attn, masked).astype(BF16)
    dk_ref[...] = dk[lead:]
    dv_ref[...] = dv[lead:]
    dkh_ref[...] = dk[:lead].astype(BF16)
    dvh_ref[...] = dv[:lead].astype(BF16)


def reduce_kernel(n_seq, entries, wg_ref, dk_ref, dv_ref, dkh_ref, dvh_ref, sq_ref, total_ref,
                  kg_ref, vg_ref, wgrad_ref, rms_ref,
                  cbuf, xsend, xbuf, rsend, rbuf, gown, gbuf, ybuf, zbuf, zsend, s_own, s_in, s_mid, s_all,
                  c_s, c_r, x_s, x_r, r_s, r_r, g_s, g_r, y_s, y_r, z_s, z_r, a_s, a_r, b_s, b_r):
    at = Place(n_seq)
    seq, dp, z, y, nz = at.seq, at.dp, at.z, at.y, at.nz
    part = wg_ref.shape[0] // n_seq
    half, quarter = part // 2, part // 4
    tok = dk_ref.shape[0]
    x = dp // 2
    meet(
        [(at.ring(1), dp), (at.ring(-1), dp), (at.y_flip(), dp)]
        + [(seq, at.dp_flip(k)) for k in (1, 2, 3)]
        + [((seq + k) % n_seq, dp) for k in range(1, n_seq)]
    )
    def quarter_row(d):
        return (d % 2) * half + (d // 2) * quarter

    def c_copy(u):
        owner = at.ring(u + 1)
        src = wg_ref.at[rows_at(owner * part + (1 - at.core) * half, half)]
        return remote(src, cbuf.at[u], c_s.at[u], c_r.at[u], seq, at.dp_flip(1))

    cc = [c_copy(u) for u in range(n_seq)]
    xc = [remote(xsend.at[u], xbuf.at[u], x_s.at[u], x_r.at[u], seq, at.dp_flip(2)) for u in range(n_seq)]
    rc = [remote(rsend.at[u], rbuf.at[u], r_s.at[u], r_r.at[u], at.ring(1), dp) for u in range(n_seq - 1)]
    halos = (dkh_ref, dvh_ref)
    down = jnp.maximum(seq - 2, y)

    def y_copy(i):
        return remote(halos[i].at[pl.ds(tok, tok)], ybuf.at[i], y_s.at[i], y_r.at[i], at.y_flip(), dp)

    def z_copy(i, summed):
        src = zsend.at[i] if summed else halos[i].at[pl.ds(0, tok)]
        return remote(src, zbuf.at[i], z_s.at[i], z_r.at[i], down, dp)

    for u in range(n_seq):
        cc[u].start()

    @pl.when((y == 1) | (z > 0))
    def _():
        for i in range(2):
            y_copy(i).start()

    @pl.when((y == 0) & (z > 0))
    def _():
        for i in range(2):
            z_copy(i, False).start()

    for u in range(n_seq):
        cc[u].wait_recv()
        first = at.ring(-u - 1) * part + at.core * half + (1 - x) * quarter
        mine = wg_ref[rows_at(first, quarter), :].astype(F32)
        theirs = cbuf[u, rows_at((1 - x) * quarter, quarter), :].astype(F32)
        xsend[u] = (mine + theirs).astype(BF16)
        xc[u].start()

    def chunk(u):
        first = at.ring(-u - 1) * part + at.core * half + x * quarter
        acc = wg_ref[rows_at(first, quarter), :].astype(F32)
        acc = acc + cbuf[u, rows_at(x * quarter, quarter), :].astype(F32)
        xc[u].wait_recv()
        acc = acc + xbuf[u].astype(F32)
        if u > 0:
            rc[u - 1].wait_recv()
            acc = acc + rbuf[u - 1].astype(F32)
        return acc

    def relay(i):
        @pl.when((y == 0) | (z > 0))
        def _():
            y_copy(i).wait_recv()

        @pl.when((y == 1) & (z > 0))
        def _():
            zsend[i] = (halos[i][0:tok, :].astype(F32) + ybuf[i].astype(F32)).astype(BF16)
            z_copy(i, True).start()

    for u in range(n_seq - 1):
        rsend[u] = chunk(u).astype(BF16)
        rc[u].start()
        if u == 1:
            relay(0)
        if u == 3:
            relay(1)

    total = total_ref[0:1, 0:1]
    act = (tok * n_seq * 4) / total
    wscale = lax.rsqrt(total)
    grads = []
    square = sq_ref[...]
    for i, (own, out) in enumerate(((dk_ref, kg_ref), (dv_ref, vg_ref))):
        @pl.when(z < nz - 1)
        def _():
            z_copy(i, False).wait_recv()

        val = own[...]
        val = val + jnp.where(y == 0, ybuf[i].astype(F32), 0.0)
        val = val + jnp.where(z < nz - 1, zbuf[i].astype(F32), 0.0)
        val = val * act
        out[...] = val.astype(BF16)
        square = square + tile_sum(val * val)

    raw = chunk(n_seq - 1)
    gown[...] = raw.astype(BF16)
    gc = [remote(gown, gbuf.at[k - 1], g_s.at[k - 1], g_r.at[k - 1], seq, at.dp_flip(k)) for k in (1, 2, 3)]
    scaled = raw * wscale
    s_own[...] = square + tile_sum(scaled * scaled)
    ac = [remote(s_own, s_in.at[k - 1], a_s.at[k - 1], a_r.at[k - 1], seq, at.dp_flip(k)) for k in (1, 2, 3)]
    for c in ac:
        c.start()
    for c in gc:
        c.start()
    for c in ac:
        c.wait_recv()
    s_mid[...] = (s_own[...] + s_in[1]) + (s_in[0] + s_in[2])
    bc = [
        remote(s_mid, s_all.at[k - 1], b_s.at[k - 1], b_r.at[k - 1], (seq + k) % n_seq, dp)
        for k in range(1, n_seq)
    ]
    for c in bc:
        c.start()
    wgrad_ref[rows_at(quarter_row(dp), quarter), :] = gown[...].astype(F32) * wscale
    for k in (1, 2, 3):
        gc[k - 1].wait_recv()
        wgrad_ref[rows_at(quarter_row(at.dp_flip(k)), quarter), :] = gbuf[k - 1].astype(F32) * wscale
    for c in bc:
        c.wait_recv()
    final = s_mid[...]
    for k in range(n_seq - 1):
        final = final + s_all[k]
    whole = jnp.sum(jnp.sum(final, axis=1, keepdims=True), axis=0, keepdims=True)
    rms_ref[...] = jnp.broadcast_to(jnp.sqrt(whole / entries), rms_ref.shape)

    for c in cc + xc + rc + gc + ac + bc:
        c.wait_send()

    @pl.when((y == 1) | (z > 0))
    def _():
        for i in range(2):
            y_copy(i).wait_send()

    @pl.when(z > 0)
    def _():
        for i in range(2):
            z_copy(i, False).wait_send()


ANY = pl.BlockSpec(memory_space=pl.ANY)
VM = pl.BlockSpec(memory_space=pltpu.VMEM)
DMA = pltpu.SemaphoreType.DMA


def fast_shards(n_seq, queries, keys, values, out_grad, out_weight, seq_len):
    q, k, v, g = queries[0], keys[0], values[0], out_grad[0]
    tok, kv_width = k.shape
    part, d_out = out_weight.shape
    width = part * n_seq
    dim, group = HEAD_DIM, HEADS // KV_HEADS
    lead = 2 * tok
    steps = n_seq - 1
    sds = jax.ShapeDtypeStruct
    length = jnp.clip(seq_len[0], 0, tok * n_seq)
    len_tile = jnp.full((8, 128), length.astype(F32), F32)
    w_full, k_halo, v_halo, total = pl.pallas_call(
        functools.partial(gather_kernel, n_seq),
        out_shape=(sds((width, d_out), BF16), sds((lead, kv_width), BF16), sds((lead, kv_width), BF16), sds((8, 128), F32)),
        in_specs=[VM, ANY, ANY, VM],
        out_specs=(ANY, ANY, ANY, VM),
        scratch_shapes=[pltpu.VMEM((3, 8, 128), F32), pltpu.VMEM((tok, kv_width), BF16)]
        + [DMA((steps,))] * 8 + [DMA((2,))] * 4 + [DMA((3,))] * 3,
        compiler_params=pltpu.CompilerParams(collective_id=0, has_side_effects=True, vmem_limit_bytes=VMEM_LIMIT),
    )(out_weight, k, v, len_tile)
    start = lax.axis_index("seq").astype(jnp.int32) * tok
    info = jnp.stack([start, seq_len[0]])
    act = (tok * n_seq * 4) / total[0:1, 0:1]
    smem = pl.BlockSpec(memory_space=pltpu.SMEM)

    def col(rows, cols):
        return pl.BlockSpec((rows, cols), lambda i: (0, i))

    dq, dk, dv, dkh, dvh, wg, sq = pl.pallas_call(
        functools.partial(attend_kernel, group),
        grid=(KV_HEADS,),
        out_shape=(
            sds((tok, width), BF16), sds((tok, kv_width), F32), sds((tok, kv_width), F32),
            sds((lead, kv_width), BF16), sds((lead, kv_width), BF16), sds((width, d_out), BF16), sds((8, 128), F32),
        ),
        in_specs=[
            smem, smem, col(tok, group * dim), col(tok, dim), col(tok, dim), col(lead, dim), col(lead, dim),
            pl.BlockSpec((tok, d_out), lambda i: (0, 0)), pl.BlockSpec((group * dim, d_out), lambda i: (i, 0)),
        ],
        out_specs=(
            col(tok, group * dim), col(tok, dim), col(tok, dim), col(lead, dim), col(lead, dim),
            pl.BlockSpec((group * dim, d_out), lambda i: (i, 0)), pl.BlockSpec((8, 128), lambda i: (0, 0)),
        ),
        scratch_shapes=[pltpu.VMEM((tok, d_out), BF16)],
        compiler_params=pltpu.CompilerParams(dimension_semantics=("arbitrary",), vmem_limit_bytes=VMEM_LIMIT),
    )(info, act, q, k, v, k_halo, v_halo, g, w_full)
    entries = tok * n_seq * 4 * (HEADS + 2 * KV_HEADS) * HEAD_DIM + width * d_out
    quarter = part // 4
    kg, vg, wgrad, rms = pl.pallas_call(
        functools.partial(reduce_kernel, n_seq, float(entries)),
        out_shape=(sds((tok, kv_width), BF16), sds((tok, kv_width), BF16), sds((part, d_out), F32), sds((8, 128), F32)),
        in_specs=[VM] * 7,
        out_specs=(VM,) * 4,
        scratch_shapes=[
            pltpu.VMEM((n_seq, part // 2, d_out), BF16),
            pltpu.VMEM((n_seq, quarter, d_out), BF16),
            pltpu.VMEM((n_seq, quarter, d_out), BF16),
            pltpu.VMEM((steps, quarter, d_out), BF16),
            pltpu.VMEM((steps, quarter, d_out), BF16),
            pltpu.VMEM((quarter, d_out), BF16),
            pltpu.VMEM((3, quarter, d_out), BF16),
            pltpu.VMEM((2, tok, kv_width), BF16),
            pltpu.VMEM((2, tok, kv_width), BF16),
            pltpu.VMEM((2, tok, kv_width), BF16),
            pltpu.VMEM((8, 128), F32),
            pltpu.VMEM((3, 8, 128), F32),
            pltpu.VMEM((8, 128), F32),
            pltpu.VMEM((steps, 8, 128), F32),
            DMA((n_seq,)), DMA((n_seq,)), DMA((n_seq,)), DMA((n_seq,)), DMA((steps,)), DMA((steps,)),
            DMA((3,)), DMA((3,)), DMA((2,)), DMA((2,)), DMA((2,)), DMA((2,)),
            DMA((3,)), DMA((3,)), DMA((steps,)), DMA((steps,)),
        ],
        compiler_params=pltpu.CompilerParams(collective_id=1, has_side_effects=True, vmem_limit_bytes=VMEM_LIMIT),
    )(wg, dk, dv, dkh, dvh, sq, total)
    return dq[None], kg[None], vg[None], wgrad, rms[0, 0]


def solution(mesh):
    n_seq, n_dp = mesh.shape["seq"], mesh.shape["dp"]
    if n_seq != HEADS or n_dp != 4:
        return plain_solution(mesh)
    row = P("dp", "seq", None)
    return jax.shard_map(
        functools.partial(fast_shards, n_seq),
        mesh=mesh,
        in_specs=(row, row, row, row, P("seq", None), P("dp")),
        out_specs=(row, row, row, P("seq", None), P()),
        check_vma=False,
    )
```
